32 devices in a mesh: dp: 2 (over x), ep: 16 (over y, z, core).
Axes of the slice: x: 2, y: 2, z: 4, core: 2. Of those that a mesh axis runs over, the one named last changes fastest.
Arguments:
- x: bfloat16 [2, 16, 512, 1280], P('dp', 'ep'), parts along dimension 0
- expert: int32 [2, 16, 512, 1], P('dp', 'ep'), parts along dimension 0
- slot: int32 [2, 16, 512, 1], P('dp', 'ep'), parts along dimension 0
- gate: float32 [2, 16, 512, 1], P('dp', 'ep'), parts along dimension 0
- w_gate: bfloat16 [32, 1280, 8192], P('ep')
- w_up: bfloat16 [32, 1280, 8192], P('ep')
- w_down: bfloat16 [32, 8192, 1280], P('ep')
- s_gate: bfloat16 [1280, 8192], replicated
- s_up: bfloat16 [1280, 8192], replicated
- s_down: bfloat16 [8192, 1280], replicated
Outputs:
- y: bfloat16 [2, 16, 512, 1280], P('dp', 'ep'), parts along dimension 0
There are 2 independent parts. The reference program is written for one: setup_inputs(seed, part) draws one part's arguments, and reference() takes and returns one part's arrays. A program takes and returns all parts, laid end to end along the dimension named above; an argument that names none is the same for every part.
All inputs are finite; a program needn't handle non-finite values.
Results may differ from the reference program's by a relative error of at most 0.009.
Values are sent between devices in bfloat16 or wider.
A program may use at most 2 GiB of HBM per device.

```python
import jax
import jax.numpy as jnp

MEMBERS = 16
TOKENS = 512
D = 1280
FF = 8192
TOP = 1
EXPERTS = 32
SHARED_FF = 8192
SLOTS = 5 * TOKENS * TOP // (4 * EXPERTS)


def setup_inputs(seed: int = 0, part: int = 0) -> dict:
    own, k1, k2, k3, k4, k5, k6 = jax.random.split(jax.random.key(seed), 7)
    kx, ke, kl, kg = jax.random.split(jax.random.fold_in(own, part), 4)
    devices = (1, MEMBERS)
    place = jax.random.permutation(kl, jnp.arange(EXPERTS, dtype=jnp.uint32))
    slow = ((EXPERTS + (9 * place) % EXPERTS) << ((9 * place) // EXPERTS)) // EXPERTS
    wait = (jax.random.bits(ke, (*devices, TOKENS, EXPERTS), jnp.uint32) >> 10) * slow
    expert = jnp.argsort(wait, axis=-1)[..., :TOP].astype(jnp.int32)
    chosen = jax.nn.one_hot(expert, EXPERTS, dtype=jnp.int32)
    in_line = jnp.cumsum(chosen.reshape(*devices, TOKENS * TOP, EXPERTS), axis=2) - 1
    slot = jnp.sum(in_line.reshape(chosen.shape) * chosen, axis=-1)

    def one(key, rows, columns):
        return (jax.random.normal(key, (rows, columns), jnp.float32) * rows**-0.5).astype(jnp.bfloat16)

    def weights(key, rows, columns):
        return jax.lax.map(lambda k: one(k, rows, columns), jax.random.split(key, EXPERTS))

    return {
        "x": jax.random.normal(kx, (*devices, TOKENS, D), jnp.float32).astype(jnp.bfloat16),
        "expert": expert,
        "slot": slot,
        "gate": jax.nn.sigmoid(jax.random.normal(kg, expert.shape, jnp.float32)),
        "w_gate": weights(k1, D, FF),
        "w_up": weights(k2, D, FF),
        "w_down": weights(k3, FF, D),
        "s_gate": one(k4, D, SHARED_FF),
        "s_up": one(k5, D, SHARED_FF),
        "s_down": one(k6, SHARED_FF, D),
    }


def einsum(form, a, b):
    return jnp.einsum(form, a.astype(jnp.float32), b.astype(jnp.float32))


def for_all(x, s_gate, s_up, s_down):
    h = jax.nn.silu(einsum("...d,df->...f", x, s_gate)) * einsum("...d,df->...f", x, s_up)
    return einsum("...f,fd->...d", h.astype(jnp.bfloat16), s_down)


def reference(x, expert, slot, gate, w_gate, w_up, w_down, s_gate, s_up, s_down):
    to_expert = jax.nn.one_hot(expert, EXPERTS, dtype=jnp.bfloat16)
    to_slot = jax.nn.one_hot(slot, SLOTS, dtype=jnp.bfloat16)
    weighted = to_expert * gate[..., None].astype(jnp.bfloat16)
    dispatch = einsum("abtke,abtkc->abtec", to_expert, to_slot).astype(jnp.bfloat16)
    combine = einsum("abtke,abtkc->abtec", weighted, to_slot).astype(jnp.bfloat16)
    z = einsum("abtec,abtd->aebcd", dispatch, x).astype(jnp.bfloat16)
    h = jax.nn.silu(einsum("aebcd,edf->aebcf", z, w_gate))
    h = (h * einsum("aebcd,edf->aebcf", z, w_up)).astype(jnp.bfloat16)
    out = einsum("aebcf,efd->aebcd", h, w_down).astype(jnp.bfloat16)
    y = einsum("abtec,aebcd->abtd", combine, out)
    return (y + for_all(x, s_gate, s_up, s_down)).astype(jnp.bfloat16)
```

```python
import functools

import jax
import jax.numpy as jnp
from jax import lax
from jax.experimental import pallas as pl
from jax.experimental.pallas import tpu as pltpu
from jax.sharding import PartitionSpec as P

MESH = pl.DeviceIdType.MESH
N = 16
SLOTS, HEAD = 20, 16
TAIL = SLOTS - HEAD
ROWS = N * SLOTS
TILE = 512
RING = 5
FIRST = 8

BF16, F32, I32 = jnp.bfloat16, jnp.float32, jnp.int32
OFFSETS = [(y, z, c) for z in (2, 1, 3, 0) for y in (1, 0) for c in (1, 0) if (y, z, c) != (0, 0, 0)]


def dot(a, b):
    return jnp.dot(a, b, preferred_element_type=F32)


def rows_of(blocks, half):
    left, right = [], []
    for s in range(N):
        left.append(blocks[s, 0:HEAD])
        right.append(blocks[s, HEAD : 2 * HEAD])
    top = lax.broadcasted_iota(I32, (2 * TAIL, half), 0) < TAIL
    for p in range(N // 2):
        a = blocks[2 * p, 2 * HEAD :].astype(F32)
        b = blocks[2 * p + 1, 2 * HEAD :].astype(F32)
        left.append(jnp.where(top, a, pltpu.roll(b, TAIL, 0)).astype(BF16))
        right.append(jnp.where(top, pltpu.roll(a, TAIL, 0), b).astype(BF16))
    return left, right


def store_rows(blocks, rows, half):
    left, right = rows_of(blocks, half)
    at = 0
    for a, b in zip(left, right):
        n = a.shape[0]
        rows[at : at + n, 0:half] = a
        rows[at : at + n, half:] = b
        at += n


def store_blocks(total, blocks, half):
    for s in range(N):
        blocks[s, 0:HEAD] = total[HEAD * s : HEAD * (s + 1), 0:half].astype(BF16)
        blocks[s, HEAD : 2 * HEAD] = total[HEAD * s : HEAD * (s + 1), half:].astype(BF16)
    top = lax.broadcasted_iota(I32, (2 * TAIL, half), 0) < TAIL
    for p in range(N // 2):
        at = N * HEAD + 2 * TAIL * p
        a = total[at : at + 2 * TAIL, 0:half]
        b = total[at : at + 2 * TAIL, half:]
        blocks[2 * p, 2 * HEAD :] = jnp.where(top, a, pltpu.roll(b, TAIL, 0)).astype(BF16)
        blocks[2 * p + 1, 2 * HEAD :] = jnp.where(top, pltpu.roll(a, TAIL, 0), b).astype(BF16)


def kernel(
    x_hbm, expert_ref, slot_ref, gate_ref, wg, wu, wd, sg, su, sd, y_ref,
    x, sent, came, back, home, z, o, total, y, ring_g, ring_u, ring_d,
    ring_sem, x_sem, go_send, go_recv, back_send, back_recv,
):
    tokens, d = x.shape
    half = d // 2
    ff = sg.shape[1]
    tile = ring_g.shape[2]
    ring = ring_g.shape[0]
    per = ff // tile
    first = per * FIRST // 16
    stretches = (
        (0, first, sg, su, sd, 0),
        (first, per, wg.at[0], wu.at[0], wd.at[0], 0),
        (first + per, per, wg.at[1], wu.at[1], wd.at[1], 0),
        (first + 2 * per, per - first, sg, su, sd, first),
    )
    steps = 3 * per

    def copies(g, u, dn, tile_index, at):
        cols = pl.ds(pl.multiple_of(tile_index * tile, tile), tile)
        return (
            pltpu.make_async_copy(g.at[:, cols], ring_g.at[at], ring_sem.at[0, at]),
            pltpu.make_async_copy(u.at[:, cols], ring_u.at[at], ring_sem.at[1, at]),
            pltpu.make_async_copy(dn.at[cols, :], ring_d.at[at], ring_sem.at[2, at]),
        )

    def fetch(step):
        at = lax.rem(step, ring)
        for lo, n, g, u, dn, skip in stretches:

            @pl.when((step >= lo) & (step < lo + n))
            def _():
                for c in copies(g, u, dn, step - lo + skip, at):
                    c.start()

    def landed(step):
        at = lax.rem(step, ring)
        for c in copies(sg, su, sd, 0, at):
            c.wait()
        return at

    load_x = pltpu.make_async_copy(x_hbm, x, x_sem)
    load_x.start()
    for step in range(ring - 1):
        for c in copies(sg, su, sd, step, step):
            c.start()
    me = lax.axis_index("ep")
    my, mz, mc = me // 8, (me // 2) % 4, me % 2
    partners = [((my + a) % 2) * 8 + ((mz + b) % 4) * 2 + (mc + c) % 2 for a, b, c in OFFSETS]
    barrier = pltpu.get_barrier_semaphore()
    for p in partners:
        pl.semaphore_signal(barrier, inc=1, device_id={"ep": p}, device_id_type=MESH)

    expert, slot = expert_ref[...], slot_ref[...]
    device = lax.shift_right_logical(expert, 1)
    which = lax.bitwise_and(expert, 1)
    head = slot < HEAD
    kept = slot < SLOTS
    head_row = jnp.where(head, device * HEAD + slot, -1)
    tail_row = jnp.where(kept & ~head, device * (2 * TAIL) + slot - HEAD, -1)
    row = jnp.where(head, head_row, jnp.where(kept, N * HEAD + device * TAIL + slot - HEAD, -1))

    def one_hot(target, e, n):
        at = lax.broadcasted_iota(I32, (n, tokens), 0)
        return (at == jnp.where(which == e, target, -1)).astype(F32).astype(BF16)

    load_x.wait()
    for e in range(2):
        heads = dot(one_hot(head_row, e, N * HEAD), x[...]).astype(BF16)
        for s in range(N):
            sent[e, s, 0:HEAD] = heads[HEAD * s : HEAD * (s + 1), 0:half]
            sent[e, s, HEAD : 2 * HEAD] = heads[HEAD * s : HEAD * (s + 1), half:]
        left = dot(one_hot(tail_row, e, N * 2 * TAIL), x[:, 0:half])
        right = dot(one_hot(jnp.where(tail_row >= 0, tail_row + TAIL, -1), e, N * 2 * TAIL), x[:, half:])
        tails = (left + right).astype(BF16)
        for s in range(N):
            sent[e, s, 2 * HEAD :] = tails[2 * TAIL * s : 2 * TAIL * (s + 1)]
        came[e, me] = sent[e, me]

    pl.semaphore_wait(barrier, len(OFFSETS))

    def remote(src, dst, e, p, send, recv):
        return pltpu.make_async_remote_copy(
            src_ref=src.at[e, p], dst_ref=dst.at[e, me], send_sem=send.at[e, p], recv_sem=recv.at[e, me],
            device_id={"ep": p}, device_id_type=MESH,
        )

    def arrived(src, dst, e, p, send, recv):
        return pltpu.make_async_remote_copy(
            src_ref=src.at[e, p], dst_ref=dst.at[e, p], send_sem=send.at[e, p], recv_sem=recv.at[e, p],
            device_id={"ep": p}, device_id_type=MESH,
        )

    for e in range(2):
        for p in partners:
            remote(sent, came, e, p, go_send, go_recv).start()

    gate = gate_ref[...].astype(BF16).astype(F32)

    def stretch(which_one, lhs, acc):
        lo, n = stretches[which_one][:2]
        acc[...] = jnp.zeros_like(acc)

        @pl.loop(0, n)
        def _(j):
            step = lo + j
            fetch(step + ring - 1)
            at = landed(step)
            a = dot(lhs[...], ring_g[at])
            b = dot(lhs[...], ring_u[at])
            h = (jax.nn.silu(a) * b).astype(BF16)
            acc[...] += dot(h, ring_d[at])

    stretch(0, x, y)
    for e in range(2):
        for p in partners:
            arrived(sent, came, e, p, go_send, go_recv).wait()
        store_rows(came.at[e], z, half)
        stretch(1 + e, z, total)
        store_blocks(total, back.at[e], half)
        home[e, me] = back[e, me]
        for p in partners:
            remote(back, home, e, p, back_send, back_recv).start()

    lo, n = stretches[3][:2]

    @pl.loop(0, n)
    def _(j):
        step = lo + j
        fetch(step + ring - 1)
        at = landed(step)
        a = dot(x[...], ring_g[at])
        b = dot(x[...], ring_u[at])
        h = (jax.nn.silu(a) * b).astype(BF16)
        y[...] += dot(h, ring_d[at])

    for e in range(2):
        at = lax.broadcasted_iota(I32, (ROWS, tokens), 0)
        pick = jnp.where(at == jnp.where(which == e, row, -1), gate, 0.0).astype(BF16)
        for p in partners:
            arrived(back, home, e, p, back_send, back_recv).wait()
        store_rows(home.at[e], o, half)
        y[...] += lax.dot_general(pick, o[...], (((0,), (0,)), ((), ())), preferred_element_type=F32)
    y_ref[...] = y[...].astype(BF16)


def layer(x, expert, slot, gate, w_gate, w_up, w_down, s_gate, s_up, s_down):
    tokens, d = x.shape[2:]
    ff = s_gate.shape[1]
    tile = min(TILE, ff // 16)
    here, there = pl.BlockSpec(memory_space=pltpu.VMEM), pl.BlockSpec(memory_space=pl.ANY)
    block = (2, N, 2 * SLOTS, d // 2)
    out = pl.pallas_call(
        kernel,
        out_shape=jax.ShapeDtypeStruct((tokens, d), BF16),
        in_specs=[there, here, here, here] + [there] * 6,
        out_specs=here,
        scratch_shapes=[
            pltpu.VMEM((tokens, d), BF16),
            pltpu.VMEM(block, BF16),
            pltpu.VMEM(block, BF16),
            pltpu.VMEM(block, BF16),
            pltpu.VMEM(block, BF16),
            pltpu.VMEM((ROWS, d), BF16),
            pltpu.VMEM((ROWS, d), BF16),
            pltpu.VMEM((ROWS, d), F32),
            pltpu.VMEM((tokens, d), F32),
            pltpu.VMEM((RING, d, tile), BF16),
            pltpu.VMEM((RING, d, tile), BF16),
            pltpu.VMEM((RING, tile, d), BF16),
            pltpu.SemaphoreType.DMA((3, RING)),
            pltpu.SemaphoreType.DMA,
            pltpu.SemaphoreType.DMA((2, N)),
            pltpu.SemaphoreType.DMA((2, N)),
            pltpu.SemaphoreType.DMA((2, N)),
            pltpu.SemaphoreType.DMA((2, N)),
        ],
        compiler_params=pltpu.CompilerParams(
            collective_id=0, has_side_effects=True, vmem_limit_bytes=60 * 1024 * 1024
        ),
        name="moe",
    )(
        x.reshape(tokens, d), expert.reshape(1, tokens), slot.reshape(1, tokens), gate.reshape(1, tokens),
        w_gate, w_up, w_down, s_gate, s_up, s_down,
    )
    return out.reshape(x.shape)


def solution(mesh):
    token = P("dp", "ep", None, None)
    weight, shared = P("ep", None, None), P(None, None)
    return jax.shard_map(
        layer,
        mesh=mesh,
        in_specs=(token,) * 4 + (weight,) * 3 + (shared,) * 3,
        out_specs=token,
        check_vma=False,
    )
```

```python
import functools

import jax
import jax.numpy as jnp
from jax import lax
from jax.experimental import pallas as pl
from jax.experimental.pallas import tpu as pltpu
from jax.sharding import PartitionSpec as P

MESH = pl.DeviceIdType.MESH
N = 16
SLOTS, HEAD = 20, 16
TAIL = SLOTS - HEAD
ROWS = N * SLOTS
TILE = 1024
RING = 5
FIRST = 8
PAIR = 2
LIMIT = 63 * 1024 * 1024

BF16, F32, I32 = jnp.bfloat16, jnp.float32, jnp.int32
OFFSETS = [(y, z, c) for z in (2, 1, 3, 0) for y in (1, 0) for c in (1, 0) if (y, z, c) != (0, 0, 0)]


def dot(a, b):
    return jnp.dot(a, b, preferred_element_type=F32)


def rows_of(blocks, half):
    left, right = [], []
    for s in range(N):
        left.append(blocks[s, 0:HEAD])
        right.append(blocks[s, HEAD : 2 * HEAD])
    top = lax.broadcasted_iota(I32, (2 * TAIL, half), 0) < TAIL
    for p in range(N // 2):
        a = blocks[2 * p, 2 * HEAD :].astype(F32)
        b = blocks[2 * p + 1, 2 * HEAD :].astype(F32)
        left.append(jnp.where(top, a, pltpu.roll(b, TAIL, 0)).astype(BF16))
        right.append(jnp.where(top, pltpu.roll(a, TAIL, 0), b).astype(BF16))
    return left, right


def store_rows(blocks, rows, half):
    left, right = rows_of(blocks, half)
    at = 0
    for a, b in zip(left, right):
        n = a.shape[0]
        rows[at : at + n, 0:half] = a
        rows[at : at + n, half:] = b
        at += n


def store_blocks(total, blocks, half):
    for s in range(N):
        blocks[s, 0:HEAD] = total[HEAD * s : HEAD * (s + 1), 0:half].astype(BF16)
        blocks[s, HEAD : 2 * HEAD] = total[HEAD * s : HEAD * (s + 1), half:].astype(BF16)
    top = lax.broadcasted_iota(I32, (2 * TAIL, half), 0) < TAIL
    for p in range(N // 2):
        at = N * HEAD + 2 * TAIL * p
        a = total[at : at + 2 * TAIL, 0:half]
        b = total[at : at + 2 * TAIL, half:]
        blocks[2 * p, 2 * HEAD :] = jnp.where(top, a, pltpu.roll(b, TAIL, 0)).astype(BF16)
        blocks[2 * p + 1, 2 * HEAD :] = jnp.where(top, pltpu.roll(a, TAIL, 0), b).astype(BF16)


def kernel(
    x_hbm, expert_ref, slot_ref, gate_ref, wg, wu, wd, sg, su, sd, y_ref,
    x, hid, sent, came, home, z, total, y, ring_g, ring_u, ring_d,
    ring_sem, x_sem, go_send, go_recv, back_send, back_recv,
):
    tokens, d = x.shape
    half = d // 2
    ff = sg.shape[1]
    tile = ring_g.shape[2]
    ring = ring_g.shape[0]
    per = ff // tile
    first = per * FIRST // 16
    stretches = (
        (0, first, sg, su, sd, 0),
        (first, per, wg.at[0], wu.at[0], wd.at[0], 0),
        (first + per, per, wg.at[1], wu.at[1], wd.at[1], 0),
        (first + 2 * per, per - first, sg, su, sd, first),
    )
    steps = 3 * per

    def copies(g, u, dn, tile_index, at):
        cols = pl.ds(pl.multiple_of(tile_index * tile, tile), tile)
        return (
            pltpu.make_async_copy(g.at[:, cols], ring_g.at[at], ring_sem.at[0, at]),
            pltpu.make_async_copy(u.at[:, cols], ring_u.at[at], ring_sem.at[1, at]),
            pltpu.make_async_copy(dn.at[cols, :], ring_d.at[at], ring_sem.at[2, at]),
        )

    def fetch(step):
        at = lax.rem(step, ring)
        for lo, n, g, u, dn, skip in stretches:

            @pl.when((step >= lo) & (step < lo + n))
            def _():
                for c in copies(g, u, dn, step - lo + skip, at):
                    c.start()

    def landed(step):
        at = lax.rem(step, ring)
        for c in copies(sg, su, sd, 0, at):
            c.wait()
        return at

    load_x = pltpu.make_async_copy(x_hbm, x, x_sem)
    load_x.start()
    me = lax.axis_index("ep")
    my, mz, mc = me // 8, (me // 2) % 4, me % 2
    partners = [((my + a) % 2) * 8 + ((mz + b) % 4) * 2 + (mc + c) % 2 for a, b, c in OFFSETS]
    barrier = pltpu.get_barrier_semaphore()
    for p in partners:
        pl.semaphore_signal(barrier, inc=1, device_id={"ep": p}, device_id_type=MESH)

    expert, slot = expert_ref[...], slot_ref[...]
    device = lax.shift_right_logical(expert, 1)
    which = lax.bitwise_and(expert, 1)
    head = slot < HEAD
    kept = slot < SLOTS
    head_row = jnp.where(head, device * HEAD + slot, -1)
    tail_row = jnp.where(kept & ~head, device * (2 * TAIL) + slot - HEAD, -1)
    row = jnp.where(head, head_row, jnp.where(kept, N * HEAD + device * TAIL + slot - HEAD, -1))

    def one_hot(target, e, n):
        at = lax.broadcasted_iota(I32, (n, tokens), 0)
        return (at == jnp.where(which == e, target, -1)).astype(F32).astype(BF16)

    def pack(e):
        heads = dot(one_hot(head_row, e, N * HEAD), x[...]).astype(BF16)
        for s in range(N):
            sent[e, s, 0:HEAD] = heads[HEAD * s : HEAD * (s + 1), 0:half]
            sent[e, s, HEAD : 2 * HEAD] = heads[HEAD * s : HEAD * (s + 1), half:]
        left = dot(one_hot(tail_row, e, N * 2 * TAIL), x[:, 0:half])
        right = dot(one_hot(jnp.where(tail_row >= 0, tail_row + TAIL, -1), e, N * 2 * TAIL), x[:, half:])
        tails = (left + right).astype(BF16)
        for s in range(N):
            sent[e, s, 2 * HEAD :] = tails[2 * TAIL * s : 2 * TAIL * (s + 1)]
        came[e, me] = sent[e, me]

    def remote(src, dst, e, p, send, recv):
        return pltpu.make_async_remote_copy(
            src_ref=src.at[e, p], dst_ref=dst.at[e, me], send_sem=send.at[e, p], recv_sem=recv.at[e, me],
            device_id={"ep": p}, device_id_type=MESH,
        )

    def arrived(src, dst, e, p, send, recv):
        return pltpu.make_async_remote_copy(
            src_ref=src.at[e, p], dst_ref=dst.at[e, p], send_sem=send.at[e, p], recv_sem=recv.at[e, p],
            device_id={"ep": p}, device_id_type=MESH,
        )

    load_x.wait()
    for step in range(ring - PAIR):
        for c in copies(sg, su, sd, step, step):
            c.start()
    pack(0)
    pl.semaphore_wait(barrier, len(OFFSETS))
    for p in partners:
        remote(sent, came, 0, p, go_send, go_recv).start()
    pack(1)

    gate = gate_ref[...].astype(BF16).astype(F32)

    def stretch(which_one, lhs, acc, fresh=True):
        lo, n = stretches[which_one][:2]
        m = lhs.shape[0]
        if fresh:
            acc[...] = jnp.zeros_like(acc)

        @pl.loop(0, n // PAIR)
        def _(j):
            step = lo + j * PAIR
            for i in range(PAIR):
                fetch(step + ring - PAIR + i)
            at = [landed(step + i) for i in range(PAIR)]
            for i in range(PAIR):
                a = dot(lhs[...], ring_g[at[i]])
                b = dot(lhs[...], ring_u[at[i]])
                hid[i, 0:m] = (jax.nn.silu(a) * b).astype(BF16)
            for i in range(PAIR):
                acc[...] += dot(hid[i, 0:m], ring_d[at[i]])

    def wait_go(e):
        for p in partners:
            arrived(sent, came, e, p, go_send, go_recv).wait()

    stretch(0, x, y)
    for e in range(2):
        wait_go(e)
        if e == 0:
            for p in partners:
                remote(sent, came, 1, p, go_send, go_recv).start()
        store_rows(came.at[e], z, half)
        stretch(1 + e, z, total)
        store_blocks(total, sent.at[e], half)
        home[e, me] = sent[e, me]
        for p in partners:
            remote(sent, home, e, p, back_send, back_recv).start()
    stretch(3, x, y, False)

    for e in range(2):
        at = lax.broadcasted_iota(I32, (ROWS, tokens), 0)
        pick = jnp.where(at == jnp.where(which == e, row, -1), gate, 0.0).astype(BF16)
        for p in partners:
            arrived(sent, home, e, p, back_send, back_recv).wait()
        store_rows(home.at[e], z, half)
        y[...] += lax.dot_general(pick, z[...], (((0,), (0,)), ((), ())), preferred_element_type=F32)
    y_ref[...] = y[...].astype(BF16)


def layer(x, expert, slot, gate, w_gate, w_up, w_down, s_gate, s_up, s_down):
    tokens, d = x.shape[2:]
    ff = s_gate.shape[1]
    tile = min(TILE, ff // 8)
    here, there = pl.BlockSpec(memory_space=pltpu.VMEM), pl.BlockSpec(memory_space=pl.ANY)
    block = (2, N, 2 * SLOTS, d // 2)
    out = pl.pallas_call(
        kernel,
        out_shape=jax.ShapeDtypeStruct((tokens, d), BF16),
        in_specs=[there, here, here, here] + [there] * 6,
        out_specs=here,
        scratch_shapes=[
            pltpu.VMEM((tokens, d), BF16),
            pltpu.VMEM((PAIR, tokens, tile), BF16),
            pltpu.VMEM(block, BF16),
            pltpu.VMEM(block, BF16),
            pltpu.VMEM(block, BF16),
            pltpu.VMEM((ROWS, d), BF16),
            pltpu.VMEM((ROWS, d), F32),
            pltpu.VMEM((tokens, d), F32),
            pltpu.VMEM((RING, d, tile), BF16),
            pltpu.VMEM((RING, d, tile), BF16),
            pltpu.VMEM((RING, tile, d), BF16),
            pltpu.SemaphoreType.DMA((3, RING)),
            pltpu.SemaphoreType.DMA,
            pltpu.SemaphoreType.DMA((2, N)),
            pltpu.SemaphoreType.DMA((2, N)),
            pltpu.SemaphoreType.DMA((2, N)),
            pltpu.SemaphoreType.DMA((2, N)),
        ],
        compiler_params=pltpu.CompilerParams(
            collective_id=0, has_side_effects=True, vmem_limit_bytes=LIMIT
        ),
        name="moe",
    )(
        x.reshape(tokens, d), expert.reshape(1, tokens), slot.reshape(1, tokens), gate.reshape(1, tokens),
        w_gate, w_up, w_down, s_gate, s_up, s_down,
    )
    return out.reshape(x.shape)


def solution(mesh):
    token = P("dp", "ep", None, None)
    weight, shared = P("ep", None, None), P(None, None)
    return jax.shard_map(
        layer,
        mesh=mesh,
        in_specs=(token,) * 4 + (weight,) * 3 + (shared,) * 3,
        out_specs=token,
        check_vma=False,
    )
```

```python
import functools

import jax
import jax.numpy as jnp
from jax import lax
from jax.experimental import pallas as pl
from jax.experimental.pallas import tpu as pltpu
from jax.sharding import PartitionSpec as P

MESH = pl.DeviceIdType.MESH
N = 16
SLOTS, HEAD = 20, 16
TAIL = SLOTS - HEAD
ROWS = N * SLOTS
TILE = 1024
RING = 5
FIRST = 8
ONE = 1
PAIR = 2
LIMIT = 63 * 1024 * 1024

BF16, F32, I32 = jnp.bfloat16, jnp.float32, jnp.int32
OFFSETS = [(y, z, c) for z in (2, 1, 3, 0) for y in (1, 0) for c in (1, 0) if (y, z, c) != (0, 0, 0)]


def dot(a, b):
    return jnp.dot(a, b, preferred_element_type=F32)


def rows_of(blocks, half):
    left, right = [], []
    for s in range(N):
        left.append(blocks[s, 0:HEAD])
        right.append(blocks[s, HEAD : 2 * HEAD])
    top = lax.broadcasted_iota(I32, (2 * TAIL, half), 0) < TAIL
    for p in range(N // 2):
        a = blocks[2 * p, 2 * HEAD :].astype(F32)
        b = blocks[2 * p + 1, 2 * HEAD :].astype(F32)
        left.append(jnp.where(top, a, pltpu.roll(b, TAIL, 0)).astype(BF16))
        right.append(jnp.where(top, pltpu.roll(a, TAIL, 0), b).astype(BF16))
    return left, right


def store_rows(blocks, rows, half):
    left, right = rows_of(blocks, half)
    at = 0
    for a, b in zip(left, right):
        n = a.shape[0]
        rows[at : at + n, 0:half] = a
        rows[at : at + n, half:] = b
        at += n


def store_blocks(total, blocks, half):
    for s in range(N):
        blocks[s, 0:HEAD] = total[HEAD * s : HEAD * (s + 1), 0:half].astype(BF16)
        blocks[s, HEAD : 2 * HEAD] = total[HEAD * s : HEAD * (s + 1), half:].astype(BF16)
    top = lax.broadcasted_iota(I32, (2 * TAIL, half), 0) < TAIL
    for p in range(N // 2):
        at = N * HEAD + 2 * TAIL * p
        a = total[at : at + 2 * TAIL, 0:half]
        b = total[at : at + 2 * TAIL, half:]
        blocks[2 * p, 2 * HEAD :] = jnp.where(top, a, pltpu.roll(b, TAIL, 0)).astype(BF16)
        blocks[2 * p + 1, 2 * HEAD :] = jnp.where(top, pltpu.roll(a, TAIL, 0), b).astype(BF16)


def kernel(
    x_hbm, expert_ref, slot_ref, gate_ref, wg, wu, wd, sg, su, sd, y_ref,
    x, hid, sent, came, home, z, total, y, ring_g, ring_u, ring_d,
    ring_sem, x_sem, go_send, go_recv, back_send, back_recv,
):
    tokens, d = x.shape
    half = d // 2
    ff = sg.shape[1]
    tile = ring_g.shape[2]
    ring = ring_g.shape[0]
    per = ff // tile
    first = per * FIRST // 16
    stretches = (
        (0, first, sg, su, sd, 0),
        (first, per, wg.at[0], wu.at[0], wd.at[0], 0),
        (first + per, per, wg.at[1], wu.at[1], wd.at[1], 0),
        (first + 2 * per, per - first, sg, su, sd, first),
    )
    steps = 3 * per

    def copies(g, u, dn, tile_index, at):
        cols = pl.ds(pl.multiple_of(tile_index * tile, tile), tile)
        return (
            pltpu.make_async_copy(g.at[:, cols], ring_g.at[at], ring_sem.at[0, at]),
            pltpu.make_async_copy(u.at[:, cols], ring_u.at[at], ring_sem.at[1, at]),
            pltpu.make_async_copy(dn.at[cols, :], ring_d.at[at], ring_sem.at[2, at]),
        )

    def fetch(step):
        at = lax.rem(step, ring)
        for lo, n, g, u, dn, skip in stretches:

            @pl.when((step >= lo) & (step < lo + n))
            def _():
                for c in copies(g, u, dn, step - lo + skip, at):
                    c.start()

    def landed(step):
        at = lax.rem(step, ring)
        for c in copies(sg, su, sd, 0, at):
            c.wait()
        return at

    load_x = pltpu.make_async_copy(x_hbm, x, x_sem)
    load_x.start()
    me = lax.axis_index("ep")
    my, mz, mc = me // 8, (me // 2) % 4, me % 2
    partners = [((my + a) % 2) * 8 + ((mz + b) % 4) * 2 + (mc + c) % 2 for a, b, c in OFFSETS]
    barrier = pltpu.get_barrier_semaphore()
    for p in partners:
        pl.semaphore_signal(barrier, inc=1, device_id={"ep": p}, device_id_type=MESH)

    expert, slot = expert_ref[...], slot_ref[...]
    device = lax.shift_right_logical(expert, 1)
    which = lax.bitwise_and(expert, 1)
    head = slot < HEAD
    kept = slot < SLOTS
    head_row = jnp.where(head, device * HEAD + slot, -1)
    tail_row = jnp.where(kept & ~head, device * (2 * TAIL) + slot - HEAD, -1)
    row = jnp.where(head, head_row, jnp.where(kept, N * HEAD + device * TAIL + slot - HEAD, -1))

    def one_hot(target, e, n):
        at = lax.broadcasted_iota(I32, (n, tokens), 0)
        return (at == jnp.where(which == e, target, -1)).astype(F32).astype(BF16)

    def pack(e):
        heads = dot(one_hot(head_row, e, N * HEAD), x[...]).astype(BF16)
        for s in range(N):
            sent[e, s, 0:HEAD] = heads[HEAD * s : HEAD * (s + 1), 0:half]
            sent[e, s, HEAD : 2 * HEAD] = heads[HEAD * s : HEAD * (s + 1), half:]
        left = dot(one_hot(tail_row, e, N * 2 * TAIL), x[:, 0:half])
        right = dot(one_hot(jnp.where(tail_row >= 0, tail_row + TAIL, -1), e, N * 2 * TAIL), x[:, half:])
        tails = (left + right).astype(BF16)
        for s in range(N):
            sent[e, s, 2 * HEAD :] = tails[2 * TAIL * s : 2 * TAIL * (s + 1)]
        came[e, me] = sent[e, me]

    def remote(src, dst, e, p, send, recv):
        return pltpu.make_async_remote_copy(
            src_ref=src.at[e, p], dst_ref=dst.at[e, me], send_sem=send.at[e, p], recv_sem=recv.at[e, me],
            device_id={"ep": p}, device_id_type=MESH,
        )

    def arrived(src, dst, e, p, send, recv):
        return pltpu.make_async_remote_copy(
            src_ref=src.at[e, p], dst_ref=dst.at[e, p], send_sem=send.at[e, p], recv_sem=recv.at[e, p],
            device_id={"ep": p}, device_id_type=MESH,
        )

    load_x.wait()
    def begin(step):
        for c in copies(sg, su, sd, step, step):
            c.start()

    begin(0)
    pack(0)
    pl.semaphore_wait(barrier, len(OFFSETS))
    for p in partners:
        remote(sent, came, 0, p, go_send, go_recv).start()
    begin(1)
    pack(1)
    for step in range(2, ring - PAIR):
        begin(step)

    gate = gate_ref[...].astype(BF16).astype(F32)

    def stretch(which_one, lhs, acc, count):
        lo, n = stretches[which_one][:2]
        m = lhs.shape[0]

        @pl.loop(0, n // count)
        def _(j):
            step = lo + j * count
            for i in range(count):
                fetch(step + ring - PAIR + i)
            at = [landed(step + i) for i in range(count)]
            for i in range(count):
                a = dot(lhs[...], ring_g[at[i]])
                b = dot(lhs[...], ring_u[at[i]])
                hid[i, 0:m] = (jax.nn.silu(a) * b).astype(BF16)
            for i in range(count):
                acc[...] += dot(hid[i, 0:m], ring_d[at[i]])

    def wait_go(e):
        for p in partners:
            arrived(sent, came, e, p, go_send, go_recv).wait()

    y[...] = jnp.zeros_like(y)
    stretch(0, x, y, ONE)
    for e in range(2):
        wait_go(e)
        if e == 0:
            for p in partners:
                remote(sent, came, 1, p, go_send, go_recv).start()
        store_rows(came.at[e], z, half)
        total[...] = jnp.zeros_like(total)
        stretch(1 + e, z, total, PAIR)
        store_blocks(total, sent.at[e], half)
        home[e, me] = sent[e, me]
        for p in partners:
            remote(sent, home, e, p, back_send, back_recv).start()
    stretch(3, x, y, PAIR)

    for e in range(2):
        at = lax.broadcasted_iota(I32, (ROWS, tokens), 0)
        pick = jnp.where(at == jnp.where(which == e, row, -1), gate, 0.0).astype(BF16)
        for p in partners:
            arrived(sent, home, e, p, back_send, back_recv).wait()
        store_rows(home.at[e], z, half)
        y[...] += lax.dot_general(pick, z[...], (((0,), (0,)), ((), ())), preferred_element_type=F32)
    y_ref[...] = y[...].astype(BF16)


def layer(x, expert, slot, gate, w_gate, w_up, w_down, s_gate, s_up, s_down):
    tokens, d = x.shape[2:]
    ff = s_gate.shape[1]
    tile = min(TILE, ff // 8)
    here, there = pl.BlockSpec(memory_space=pltpu.VMEM), pl.BlockSpec(memory_space=pl.ANY)
    block = (2, N, 2 * SLOTS, d // 2)
    out = pl.pallas_call(
        kernel,
        out_shape=jax.ShapeDtypeStruct((tokens, d), BF16),
        in_specs=[there, here, here, here] + [there] * 6,
        out_specs=here,
        scratch_shapes=[
            pltpu.VMEM((tokens, d), BF16),
            pltpu.VMEM((PAIR, tokens, tile), BF16),
            pltpu.VMEM(block, BF16),
            pltpu.VMEM(block, BF16),
            pltpu.VMEM(block, BF16),
            pltpu.VMEM((ROWS, d), BF16),
            pltpu.VMEM((ROWS, d), F32),
            pltpu.VMEM((tokens, d), F32),
            pltpu.VMEM((RING, d, tile), BF16),
            pltpu.VMEM((RING, d, tile), BF16),
            pltpu.VMEM((RING, tile, d), BF16),
            pltpu.SemaphoreType.DMA((3, RING)),
            pltpu.SemaphoreType.DMA,
            pltpu.SemaphoreType.DMA((2, N)),
            pltpu.SemaphoreType.DMA((2, N)),
            pltpu.SemaphoreType.DMA((2, N)),
            pltpu.SemaphoreType.DMA((2, N)),
        ],
        compiler_params=pltpu.CompilerParams(
            collective_id=0, has_side_effects=True, vmem_limit_bytes=LIMIT
        ),
        name="moe",
    )(
        x.reshape(tokens, d), expert.reshape(1, tokens), slot.reshape(1, tokens), gate.reshape(1, tokens),
        w_gate, w_up, w_down, s_gate, s_up, s_down,
    )
    return out.reshape(x.shape)


def solution(mesh):
    token = P("dp", "ep", None, None)
    weight, shared = P("ep", None, None), P(None, None)
    return jax.shard_map(
        layer,
        mesh=mesh,
        in_specs=(token,) * 4 + (weight,) * 3 + (shared,) * 3,
        out_specs=token,
        check_vma=False,
    )
```
